64 devices in a mesh: dp: 4 (over x, y), ep: 16 (over z, core).
Axes of the slice: x: 2, y: 2, z: 8, core: 2. Of those that a mesh axis runs over, the one named last changes fastest.
The devices are a block of a 4x4x8 slice.
Arguments:
- x_a: bfloat16 [16384, 2048], P(('dp', 'ep')), parts along dimension 0
- route_a: int32 [16384, 8], P(('dp', 'ep')), parts along dimension 0
- gate_a: float32 [16384, 8], P(('dp', 'ep')), parts along dimension 0
- h_b: bfloat16 [16384, 2048], P(('dp', 'ep')), parts along dimension 0
- attn_b: bfloat16 [16384, 2048], P(('dp', 'ep')), parts along dimension 0
- route_b: int32 [16384, 8], P(('dp', 'ep')), parts along dimension 0
- gate_b: float32 [16384, 8], P(('dp', 'ep')), parts along dimension 0
- w_qkv: bfloat16 [2048, 6144], replicated
- w_o: bfloat16 [2048, 2048], replicated
- w_gate: bfloat16 [64, 2048, 1024], P('ep')
- w_up: bfloat16 [64, 2048, 1024], P('ep')
- w_down: bfloat16 [64, 1024, 2048], P('ep')
Outputs:
- output 1: bfloat16 [16384, 2048], P(('dp', 'ep')), parts along dimension 0
- output 2: bfloat16 [16384, 2048], P(('dp', 'ep')), parts along dimension 0
- output 3: bfloat16 [16384, 6144], P(('dp', 'ep')), parts along dimension 0
There are 4 independent parts. The reference program is written for one: setup_inputs(seed, part) draws one part's arguments, and reference() takes and returns one part's arrays. A program takes and returns all parts, laid end to end along the dimension named above; an argument that names none is the same for every part.
All inputs are finite; a program needn't handle non-finite values.
Results may differ from the reference program's by a relative error of at most 0.0107879.
Values are sent between devices in bfloat16 or wider.
A program may use at most 768 MiB of HBM per device.

```python
import jax
import jax.numpy as jnp
from jax import lax

MODEL_DIM = 2048
FF_DIM = 1024
NUM_EXPERTS = 64
TOP_K = 8
NUM_HEADS = 16
KV_HEADS = 16
HEAD_DIM = 128
TOKENS_DEV = 256
GROUP_DEVS = 16

CAPACITY = min(TOKENS_DEV, 2 * ((TOKENS_DEV * TOP_K + NUM_EXPERTS - 1) // NUM_EXPERTS))
LOCAL_EXPERTS = NUM_EXPERTS // GROUP_DEVS
QKV_DIM = (NUM_HEADS + 2 * KV_HEADS) * HEAD_DIM
ATTN_DIM = NUM_HEADS * HEAD_DIM
GROUP_ROWS = GROUP_DEVS * TOKENS_DEV
HOT_DEVS = max(1, GROUP_DEVS // 4)


def source_routing(rng_key, dev_order):
    key_local, key_want, key_rows = jax.random.split(rng_key, 3)
    local_order = jax.vmap(lambda sub_key: jax.random.permutation(sub_key, LOCAL_EXPERTS))(jax.random.split(key_local, GROUP_DEVS))
    visits = jnp.arange(NUM_EXPERTS)
    visit_dev = dev_order[visits % GROUP_DEVS]
    visit_expert = visit_dev * LOCAL_EXPERTS + local_order[visit_dev, visits // GROUP_DEVS]
    wanted = jax.random.randint(key_want, (NUM_EXPERTS,), 1, CAPACITY + 1)
    wanted = jnp.where(visits % GROUP_DEVS < HOT_DEVS, CAPACITY, wanted)
    wanted = jnp.where(visits < GROUP_DEVS, 1, wanted)
    wanted = jnp.where(visits == 0, CAPACITY, wanted)
    n_entries = TOKENS_DEV * TOP_K
    first_pass = jnp.clip(n_entries - (jnp.cumsum(wanted) - wanted), 0, wanted)
    room_left = CAPACITY - first_pass
    left_over = n_entries - jnp.sum(first_pass)
    second_pass = jnp.clip(left_over - (jnp.cumsum(room_left) - room_left), 0, room_left)
    run_ends = jnp.cumsum(first_pass + second_pass)
    positions = jnp.arange(n_entries)
    run_index = jnp.sum((run_ends[None, :] <= positions[:, None]).astype(jnp.int32), axis=1)
    choices = visit_expert[run_index].reshape(TOP_K, TOKENS_DEV).T
    return choices[jax.random.permutation(key_rows, TOKENS_DEV)]


def group_routing(rng_key):
    key_order, key_src = jax.random.split(rng_key)
    dev_order = jax.random.permutation(key_order, GROUP_DEVS)
    per_source = jax.vmap(lambda sub_key: source_routing(sub_key, dev_order))(jax.random.split(key_src, GROUP_DEVS))
    return per_source.reshape(GROUP_ROWS, TOP_K).astype(jnp.int32)


def setup_inputs(seed: int = 0, part: int = 0) -> dict:
    root_key = jax.random.key(seed)
    shared_keys = jax.random.split(jax.random.fold_in(root_key, 1), 5)
    part_keys = jax.random.split(jax.random.fold_in(jax.random.fold_in(root_key, 2), part), 7)

    def normal_bf16(sub_key, arr_shape, scale_by):
        return (jax.random.normal(sub_key, arr_shape, jnp.float32) * scale_by).astype(jnp.bfloat16)

    return {
        'x_a': normal_bf16(part_keys[0], (GROUP_ROWS, MODEL_DIM), 1.0),
        'route_a': group_routing(part_keys[1]),
        'gate_a': jax.nn.softmax(jax.random.normal(part_keys[2], (GROUP_ROWS, TOP_K), jnp.float32), axis=-1),
        'h_b': normal_bf16(part_keys[3], (GROUP_ROWS, MODEL_DIM), 1.0),
        'attn_b': normal_bf16(part_keys[4], (GROUP_ROWS, ATTN_DIM), 1.0),
        'route_b': group_routing(part_keys[5]),
        'gate_b': jax.nn.softmax(jax.random.normal(part_keys[6], (GROUP_ROWS, TOP_K), jnp.float32), axis=-1),
        'w_qkv': normal_bf16(shared_keys[0], (MODEL_DIM, QKV_DIM), MODEL_DIM ** -0.5),
        'w_o': normal_bf16(shared_keys[1], (ATTN_DIM, MODEL_DIM), ATTN_DIM ** -0.5),
        'w_gate': normal_bf16(shared_keys[2], (NUM_EXPERTS, MODEL_DIM, FF_DIM), MODEL_DIM ** -0.5),
        'w_up': normal_bf16(shared_keys[3], (NUM_EXPERTS, MODEL_DIM, FF_DIM), MODEL_DIM ** -0.5),
        'w_down': normal_bf16(shared_keys[4], (NUM_EXPERTS, FF_DIM, MODEL_DIM), FF_DIM ** -0.5),
    }


def expert_layer(tokens, route_ids, gate_vals, w_gate, w_up, w_down):
    n_entries = GROUP_ROWS * TOP_K
    per_source = route_ids.reshape(GROUP_DEVS, TOKENS_DEV * TOP_K)
    one_hot = (per_source[:, :, None] == jnp.arange(NUM_EXPERTS)[None, None, :]).astype(jnp.int32)
    slot_rank = jnp.sum((jnp.cumsum(one_hot, axis=1) - 1) * one_hot, axis=2)
    buffer_row = jnp.arange(GROUP_DEVS)[:, None] * CAPACITY + slot_rank
    entry_ids = jnp.arange(n_entries)
    slot_table = jnp.full((NUM_EXPERTS, GROUP_DEVS * CAPACITY), n_entries, jnp.int32)
    slot_table = slot_table.at[per_source.reshape(-1), buffer_row.reshape(-1)].set(entry_ids)
    padded = jnp.concatenate([tokens, jnp.zeros((1, MODEL_DIM), tokens.dtype)], axis=0)

    def one_expert(results, inputs):
        rows_ids, gate_w, up_w, down_w = inputs
        expert_in = padded[rows_ids // TOP_K]
        gate_act = jnp.dot(expert_in, gate_w, preferred_element_type=jnp.float32)
        up_act = jnp.dot(expert_in, up_w, preferred_element_type=jnp.float32)
        hidden = (jax.nn.silu(gate_act) * up_act).astype(jnp.bfloat16)
        expert_out = jnp.dot(hidden, down_w, preferred_element_type=jnp.float32).astype(jnp.bfloat16)
        return results.at[rows_ids].set(expert_out), None

    results = jnp.zeros((n_entries + 1, MODEL_DIM), jnp.bfloat16)
    results = lax.scan(one_expert, results, (slot_table, w_gate, w_up, w_down))[0]
    per_choice = results[:n_entries].reshape(GROUP_ROWS, TOP_K, MODEL_DIM)
    mixture = jnp.zeros((GROUP_ROWS, MODEL_DIM), jnp.float32)
    for choice in range(TOP_K):
        mixture = mixture + gate_vals[:, choice:choice + 1] * per_choice[:, choice].astype(jnp.float32)
    return (tokens.astype(jnp.float32) + mixture).astype(jnp.bfloat16)


def reference(x_a, route_a, gate_a, h_b, attn_b, route_b, gate_b, w_qkv, w_o, w_gate, w_up, w_down):
    out_a = expert_layer(x_a, route_a, gate_a, w_gate, w_up, w_down)
    qkv_b = jnp.dot(h_b, w_qkv, preferred_element_type=jnp.float32).astype(jnp.bfloat16)
    proj_b = jnp.dot(attn_b, w_o, preferred_element_type=jnp.float32).astype(jnp.bfloat16)
    mid_b = (h_b.astype(jnp.float32) + proj_b.astype(jnp.float32)).astype(jnp.bfloat16)
    out_b = expert_layer(mid_b, route_b, gate_b, w_gate, w_up, w_down)
    return (out_a, out_b, qkv_b)
```

```python
import functools

import jax
import jax.numpy as jnp
from jax import lax
from jax.experimental import pallas as pl
from jax.experimental.pallas import tpu as pltpu
from jax.sharding import PartitionSpec as P

CORES = 2


def slot_tables(route_all, gate_all, expert_ids):
    n_src, tok_n, top_k = route_all.shape
    route_t = jnp.swapaxes(route_all, 1, 2)
    gate_t = jnp.swapaxes(gate_all, 1, 2)
    hit = route_t[:, :, None, :] == expert_ids[None, None, :, None]
    chosen = jnp.any(hit, axis=1)
    gate = jnp.sum(jnp.where(hit, gate_t[:, :, None, :], 0.0), axis=1)
    before = (jnp.arange(tok_n)[:, None] < jnp.arange(tok_n)[None, :]).astype(jnp.bfloat16)
    rank = jnp.einsum('set,tu->seu', chosen.astype(jnp.bfloat16), before, preferred_element_type=jnp.float32)
    rank = jnp.where(chosen, rank.astype(jnp.int32), -1)
    return rank, jnp.swapaxes(rank, 1, 2), jnp.swapaxes(gate, 1, 2)


def moe_kernel(n_src, local_n, capacity, rank_ref, rank_t_ref, gate_ref, x_ref, *refs):
    own, peer = refs[0:3], refs[3:6]
    out_ref, rows_ref = refs[6], refs[7]
    bufs, sems = refs[8:11], refs[11]
    n_exp = CORES * local_n
    step = pl.program_id(0)
    tok_n, model_dim = x_ref.shape[1:]

    def load(side, idx, slot):
        for k in range(3):
            pltpu.make_async_copy(side[k].at[idx], bufs[k].at[slot], sems.at[slot, k]).start()

    @pl.when(step == 0)
    def _():
        load(own, 0, 0)
        load(own, 1, 1)

    @pl.when(step < n_src)
    def _():
        slot_no = lax.broadcasted_iota(jnp.int32, (capacity, tok_n), 0)
        picks = [jnp.where(slot_no == rank_ref[0, e : e + 1, :], 1.0, 0.0) for e in range(n_exp)]
        place = jnp.concatenate(picks, axis=0).astype(jnp.bfloat16)
        rows_ref[step] = jnp.dot(place, x_ref[0], preferred_element_type=jnp.float32).astype(jnp.bfloat16)

    @pl.when(jnp.logical_and(step >= n_src, step < n_src + n_exp))
    def _():
        e = step - n_src
        slot = lax.rem(e, 2)
        for k in range(3):
            pltpu.make_async_copy(own[k].at[0], bufs[k].at[slot], sems.at[slot, k]).wait()
        at = pl.ds(pl.multiple_of(e * capacity, capacity), capacity)
        rows = rows_ref[:, at, :].reshape(n_src * capacity, model_dim)
        gate_act = jnp.dot(rows, bufs[0][slot], preferred_element_type=jnp.float32)
        up_act = jnp.dot(rows, bufs[1][slot], preferred_element_type=jnp.float32)
        hidden = (gate_act * jax.nn.sigmoid(gate_act) * up_act).astype(jnp.bfloat16)
        y = jnp.dot(hidden, bufs[2][slot], preferred_element_type=jnp.float32).astype(jnp.bfloat16)
        rows_ref[:, at, :] = y.reshape(n_src, capacity, model_dim)

        @pl.when(e + 2 < local_n)
        def _():
            load(own, e + 2, slot)

        @pl.when(jnp.logical_and(e + 2 >= local_n, e + 2 < n_exp))
        def _():
            load(peer, e + 2 - local_n, slot)

    @pl.when(step >= n_src + n_exp)
    def _():
        src = step - n_src - n_exp
        col = lax.broadcasted_iota(jnp.int32, (tok_n, capacity), 1)
        parts = []
        for e in range(n_exp):
            parts.append(jnp.where(col == rank_t_ref[0, :, e : e + 1], gate_ref[0, :, e : e + 1], 0.0))
        weight = jnp.concatenate(parts, axis=1)
        hi = weight.astype(jnp.bfloat16)
        rest = weight - hi.astype(jnp.float32)
        mid = rest.astype(jnp.bfloat16)
        lo = (rest - mid.astype(jnp.float32)).astype(jnp.bfloat16)
        y = rows_ref[src]
        total = jnp.dot(hi, y, preferred_element_type=jnp.float32)
        total += jnp.dot(mid, y, preferred_element_type=jnp.float32)
        total += jnp.dot(lo, y, preferred_element_type=jnp.float32)
        out_ref[0] = total


def expert_sums(rows_all, tables, own, peer):
    n_src, tok_n, model_dim = rows_all.shape
    local_n, _, ff_dim = own[0].shape
    n_exp = CORES * local_n
    rank, rank_t, gate = tables
    n_devs = n_src * CORES
    capacity = min(tok_n, 2 * ((tok_n * 8 + n_devs * local_n - 1) // (n_devs * local_n)))
    first = lambda i: (jnp.minimum(i, n_src - 1), 0, 0)
    last = lambda i: (jnp.clip(i - n_src - n_exp, 0, n_src - 1), 0, 0)
    any_spec = pl.BlockSpec(memory_space=pl.ANY)
    slots = n_exp * capacity
    flops = n_src * slots * model_dim * (6 * ff_dim + 2 * tok_n * 4)
    return pl.pallas_call(
        functools.partial(moe_kernel, n_src, local_n, capacity),
        grid=(n_src + n_exp + n_src,),
        out_shape=jax.ShapeDtypeStruct((n_src, tok_n, model_dim), jnp.float32),
        in_specs=[
            pl.BlockSpec((1, n_exp, tok_n), first),
            pl.BlockSpec((1, tok_n, n_exp), last),
            pl.BlockSpec((1, tok_n, n_exp), last),
            pl.BlockSpec((1, tok_n, model_dim), first),
        ]
        + [any_spec] * 6,
        out_specs=pl.BlockSpec((1, tok_n, model_dim), last),
        scratch_shapes=[
            pltpu.VMEM((n_src, slots, model_dim), jnp.bfloat16),
            pltpu.VMEM((2, model_dim, ff_dim), jnp.bfloat16),
            pltpu.VMEM((2, model_dim, ff_dim), jnp.bfloat16),
            pltpu.VMEM((2, ff_dim, model_dim), jnp.bfloat16),
            pltpu.SemaphoreType.DMA((2, 3)),
        ],
        compiler_params=pltpu.CompilerParams(
            dimension_semantics=('arbitrary',), vmem_limit_bytes=62 * 1024 * 1024
        ),
        cost_estimate=pl.CostEstimate(flops=flops, bytes_accessed=160 * 2**20, transcendentals=0),
    )(rank, rank_t, gate, rows_all, *own, *peer)


def solution(mesh):
    n_devs = mesh.shape['ep']
    groups = [list(range(c, n_devs, CORES)) for c in range(CORES)]
    swap = [(d, d ^ 1) for d in range(n_devs)]

    def gather(vals):
        return lax.all_gather(vals, 'ep', axis_index_groups=groups)

    def local_step(x_a, route_a, gate_a, h_b, attn_b, route_b, gate_b, w_qkv, w_o, w_gate, w_up, w_down):
        k = route_a.shape[1]
        local_n = w_gate.shape[0]
        me = lax.axis_index('ep')
        own = (w_gate, w_up, w_down)
        rows_a = gather(x_a)
        peer = tuple(lax.ppermute(w, 'ep', swap) for w in own)
        proj_b = jnp.dot(attn_b, w_o, preferred_element_type=jnp.float32).astype(jnp.bfloat16)
        mid_b = (h_b.astype(jnp.float32) + proj_b.astype(jnp.float32)).astype(jnp.bfloat16)
        rows_a, sent_b = lax.optimization_barrier((rows_a, mid_b))
        rows_b = gather(sent_b)
        meta = jnp.concatenate([route_a.astype(jnp.float32), gate_a, route_b.astype(jnp.float32), gate_b], axis=1)
        meta = gather(meta)
        ids = meta.astype(jnp.int32)
        local = jnp.arange(local_n)
        expert_ids = jnp.concatenate([me * local_n + local, (me ^ 1) * local_n + local])
        tables_a = slot_tables(ids[:, :, :k], meta[:, :, k : 2 * k], expert_ids)
        tables_b = slot_tables(ids[:, :, 2 * k : 3 * k], meta[:, :, 3 * k :], expert_ids)
        part_a = expert_sums(rows_a, tables_a, own, peer)
        sum_a = lax.psum_scatter(part_a, 'ep', axis_index_groups=groups)
        part_b = expert_sums(rows_b, tables_b, own, peer)
        sum_b = lax.psum_scatter(part_b, 'ep', axis_index_groups=groups)
        qkv_b = jnp.dot(h_b, w_qkv, preferred_element_type=jnp.float32).astype(jnp.bfloat16)
        out_a = (x_a.astype(jnp.float32) + sum_a).astype(jnp.bfloat16)
        out_b = (mid_b.astype(jnp.float32) + sum_b).astype(jnp.bfloat16)
        return out_a, out_b, qkv_b

    row_spec = P(('dp', 'ep'), None)
    full_spec = P(None, None)
    expert_spec = P('ep', None, None)
    return jax.shard_map(
        local_step,
        mesh=mesh,
        in_specs=(row_spec, row_spec, row_spec, row_spec, row_spec, row_spec, row_spec, full_spec, full_spec, expert_spec, expert_spec, expert_spec),
        out_specs=(row_spec, row_spec, row_spec),
        check_vma=False,
    )
```

```python
import functools

import jax
import jax.numpy as jnp
from jax import lax
from jax.experimental import pallas as pl
from jax.experimental.pallas import tpu as pltpu
from jax.sharding import PartitionSpec as P

CORES = 2


def slot_tables(route_all, gate_all, expert_ids):
    n_src, tok_n, top_k = route_all.shape
    route_t = jnp.swapaxes(route_all, 1, 2)
    gate_t = jnp.swapaxes(gate_all, 1, 2)
    hit = route_t[:, :, None, :] == expert_ids[None, None, :, None]
    chosen = jnp.any(hit, axis=1)
    gate = jnp.sum(jnp.where(hit, gate_t[:, :, None, :], 0.0), axis=1)
    before = (jnp.arange(tok_n)[:, None] < jnp.arange(tok_n)[None, :]).astype(jnp.bfloat16)
    rank = jnp.einsum('set,tu->seu', chosen.astype(jnp.bfloat16), before, preferred_element_type=jnp.float32)
    rank = jnp.where(chosen, rank.astype(jnp.int32), -1)
    return rank, jnp.swapaxes(rank, 1, 2), jnp.swapaxes(gate, 1, 2)


def moe_kernel(n_src, local_n, capacity, rank_ref, rank_t_ref, gate_ref, x_ref, *refs):
    own, peer = refs[0:3], refs[3:6]
    out_ref, rows_ref = refs[6], refs[7]
    bufs, sems = refs[8:11], refs[11]
    n_exp = CORES * local_n
    step = pl.program_id(0)
    tok_n, model_dim = x_ref.shape[1:]

    def load(side, idx, slot):
        for k in range(3):
            pltpu.make_async_copy(side[k].at[idx], bufs[k].at[slot], sems.at[slot, k]).start()

    @pl.when(step == 0)
    def _():
        load(own, 0, 0)
        load(own, 1, 1)

    @pl.when(step < n_src)
    def _():
        slot_no = lax.broadcasted_iota(jnp.int32, (capacity, tok_n), 0)
        picks = [jnp.where(slot_no == rank_ref[0, e : e + 1, :], 1.0, 0.0) for e in range(n_exp)]
        place = jnp.concatenate(picks, axis=0).astype(jnp.bfloat16)
        rows_ref[step] = jnp.dot(place, x_ref[0], preferred_element_type=jnp.float32).astype(jnp.bfloat16)

    @pl.when(jnp.logical_and(step >= n_src, step < n_src + n_exp))
    def _():
        e = step - n_src
        slot = lax.rem(e, 2)
        for k in range(3):
            pltpu.make_async_copy(own[k].at[0], bufs[k].at[slot], sems.at[slot, k]).wait()
        at = pl.ds(pl.multiple_of(e * capacity, capacity), capacity)
        rows = rows_ref[:, at, :].reshape(n_src * capacity, model_dim)
        gate_act = jnp.dot(rows, bufs[0][slot], preferred_element_type=jnp.float32)
        up_act = jnp.dot(rows, bufs[1][slot], preferred_element_type=jnp.float32)
        hidden = (gate_act * jax.nn.sigmoid(gate_act) * up_act).astype(jnp.bfloat16)
        y = jnp.dot(hidden, bufs[2][slot], preferred_element_type=jnp.float32).astype(jnp.bfloat16)
        rows_ref[:, at, :] = y.reshape(n_src, capacity, model_dim)

        @pl.when(e + 2 < local_n)
        def _():
            load(own, e + 2, slot)

        @pl.when(jnp.logical_and(e + 2 >= local_n, e + 2 < n_exp))
        def _():
            load(peer, e + 2 - local_n, slot)

    @pl.when(step >= n_src + n_exp)
    def _():
        src = step - n_src - n_exp
        col = lax.broadcasted_iota(jnp.int32, (tok_n, capacity), 1)
        parts = []
        for e in range(n_exp):
            parts.append(jnp.where(col == rank_t_ref[0, :, e : e + 1], gate_ref[0, :, e : e + 1], 0.0))
        weight = jnp.concatenate(parts, axis=1)
        hi = weight.astype(jnp.bfloat16)
        rest = weight - hi.astype(jnp.float32)
        mid = rest.astype(jnp.bfloat16)
        lo = (rest - mid.astype(jnp.float32)).astype(jnp.bfloat16)
        y = rows_ref[src]
        total = jnp.dot(hi, y, preferred_element_type=jnp.float32)
        total += jnp.dot(mid, y, preferred_element_type=jnp.float32)
        total += jnp.dot(lo, y, preferred_element_type=jnp.float32)
        out_ref[0] = total


def expert_sums(rows_all, tables, own, peer):
    n_src, tok_n, model_dim = rows_all.shape
    local_n, _, ff_dim = own[0].shape
    n_exp = CORES * local_n
    rank, rank_t, gate = tables
    n_devs = n_src * CORES
    capacity = min(tok_n, 2 * ((tok_n * 8 + n_devs * local_n - 1) // (n_devs * local_n)))
    first = lambda i: (jnp.minimum(i, n_src - 1), 0, 0)
    last = lambda i: (jnp.clip(i - n_src - n_exp, 0, n_src - 1), 0, 0)
    any_spec = pl.BlockSpec(memory_space=pl.ANY)
    slots = n_exp * capacity
    flops = n_src * slots * model_dim * (6 * ff_dim + 2 * tok_n * 4)
    return pl.pallas_call(
        functools.partial(moe_kernel, n_src, local_n, capacity),
        grid=(n_src + n_exp + n_src,),
        out_shape=jax.ShapeDtypeStruct((n_src, tok_n, model_dim), jnp.float32),
        in_specs=[
            pl.BlockSpec((1, n_exp, tok_n), first),
            pl.BlockSpec((1, tok_n, n_exp), last),
            pl.BlockSpec((1, tok_n, n_exp), last),
            pl.BlockSpec((1, tok_n, model_dim), first),
        ]
        + [any_spec] * 6,
        out_specs=pl.BlockSpec((1, tok_n, model_dim), last),
        scratch_shapes=[
            pltpu.VMEM((n_src, slots, model_dim), jnp.bfloat16),
            pltpu.VMEM((2, model_dim, ff_dim), jnp.bfloat16),
            pltpu.VMEM((2, model_dim, ff_dim), jnp.bfloat16),
            pltpu.VMEM((2, ff_dim, model_dim), jnp.bfloat16),
            pltpu.SemaphoreType.DMA((2, 3)),
        ],
        compiler_params=pltpu.CompilerParams(
            dimension_semantics=('arbitrary',), vmem_limit_bytes=62 * 1024 * 1024
        ),
        cost_estimate=pl.CostEstimate(flops=flops, bytes_accessed=160 * 2**20, transcendentals=0),
    )(rank, rank_t, gate, rows_all, *own, *peer)


def ring_kernel(n_src, n_devs, part_ref, mid_ref, out_ref, local, slots, load_sems, send_sems, recv_sems):
    tok_n, model_dim = mid_ref.shape
    rows_n, cols_n = tok_n // 2, model_dim // 2
    me = lax.axis_index('ep')
    pos = lax.div(me, CORES)
    to = {1: lax.rem(me + CORES, n_devs), -1: lax.rem(me + n_devs - CORES, n_devs)}

    barrier = pltpu.get_barrier_semaphore()
    for way in (1, -1):
        pl.semaphore_signal(barrier, inc=1, device_id={'ep': to[way]}, device_id_type=pl.DeviceIdType.MESH)
    pl.semaphore_wait(barrier, 2)

    far = n_src // 2
    near = n_src - 1 - far
    chains = []
    for dist, pairs in ((far, ((1, 0), (-1, 1))), (near, ((1, 1), (-1, 0)))):
        for r in range(2):
            for way, h in pairs:
                chains.append((way, r, h, dist))
    base, count = [], 0
    for chain in chains:
        base.append(count)
        count += chain[3]

    loads = {}
    order = sorted(range(n_src), key=lambda j: -min(j, n_src - j))
    for j in order:
        loads[j] = pltpu.make_async_copy(part_ref.at[lax.rem(pos + j, n_src)], local.at[j], load_sems.at[j])
        loads[j].start()
    ready = set()

    def mine(way, dist, r, h):
        j = (way * dist) % n_src
        if j not in ready:
            loads[j].wait()
            ready.add(j)
        return local.at[j, pl.ds(r * rows_n, rows_n), pl.ds(h * cols_n, cols_n)]

    copies = {}

    def send(c, hop, src):
        at = base[c] + hop - 1
        copies[c, hop] = pltpu.make_async_remote_copy(
            src_ref=src,
            dst_ref=slots.at[at],
            send_sem=send_sems.at[at],
            recv_sem=recv_sems.at[at],
            device_id={'ep': to[chains[c][0]]},
            device_id_type=pl.DeviceIdType.MESH,
        )
        copies[c, hop].start()

    for c, (way, r, h, dist) in enumerate(chains):
        send(c, 1, mine(way, dist, r, h))
    landed = {}
    for hop in range(1, far + 1):
        for c, (way, r, h, dist) in enumerate(chains):
            if hop > dist:
                continue
            copies[c, hop].wait_recv()
            here = slots.at[base[c] + hop - 1]
            if hop < dist:
                here[...] += mine(way, dist - hop, r, h)[...]
                send(c, hop + 1, here)
                continue
            if (r, h) not in landed:
                landed[r, h] = here
                continue
            total = mine(1, 0, r, h)[...] + (landed[r, h][...] + here[...])
            spot = (pl.ds(r * rows_n, rows_n), pl.ds(h * cols_n, cols_n))
            out_ref[spot] = (mid_ref[spot].astype(jnp.float32) + total).astype(jnp.bfloat16)
    for copy in copies.values():
        copy.wait_send()


def ring_sum(part, mid, n_devs):
    n_src, tok_n, model_dim = part.shape
    n_slots = 2 * 2 * (n_src - 1)
    vmem = pl.BlockSpec(memory_space=pltpu.VMEM)
    return pl.pallas_call(
        functools.partial(ring_kernel, n_src, n_devs),
        out_shape=jax.ShapeDtypeStruct((tok_n, model_dim), jnp.bfloat16),
        in_specs=[pl.BlockSpec(memory_space=pl.ANY), vmem],
        out_specs=vmem,
        scratch_shapes=[
            pltpu.VMEM((n_src, tok_n, model_dim), jnp.float32),
            pltpu.VMEM((n_slots, tok_n // 2, model_dim // 2), jnp.float32),
            pltpu.SemaphoreType.DMA((n_src,)),
            pltpu.SemaphoreType.DMA((n_slots,)),
            pltpu.SemaphoreType.DMA((n_slots,)),
        ],
        compiler_params=pltpu.CompilerParams(
            collective_id=0, has_side_effects=True, vmem_limit_bytes=56 * 1024 * 1024
        ),
        cost_estimate=pl.CostEstimate(flops=80 * 10**9, bytes_accessed=20 * 2**20, transcendentals=0),
    )(part, mid)


def solution(mesh):
    n_devs = mesh.shape['ep']
    groups = [list(range(c, n_devs, CORES)) for c in range(CORES)]
    swap = [(d, d ^ 1) for d in range(n_devs)]

    def gather(vals):
        return lax.all_gather(vals, 'ep', axis_index_groups=groups)

    def local_step(x_a, route_a, gate_a, h_b, attn_b, route_b, gate_b, w_qkv, w_o, w_gate, w_up, w_down):
        k = route_a.shape[1]
        local_n = w_gate.shape[0]
        me = lax.axis_index('ep')
        own = (w_gate, w_up, w_down)
        rows_a = gather(x_a)
        peer = tuple(lax.ppermute(w, 'ep', swap) for w in own)
        proj_b = jnp.dot(attn_b, w_o, preferred_element_type=jnp.float32).astype(jnp.bfloat16)
        mid_b = (h_b.astype(jnp.float32) + proj_b.astype(jnp.float32)).astype(jnp.bfloat16)
        meta = jnp.concatenate([route_a.astype(jnp.float32), gate_a, route_b.astype(jnp.float32), gate_b], axis=1)
        meta = gather(meta)
        ids = meta.astype(jnp.int32)
        local = jnp.arange(local_n)
        expert_ids = jnp.concatenate([me * local_n + local, (me ^ 1) * local_n + local])
        tables_a = slot_tables(ids[:, :, :k], meta[:, :, k : 2 * k], expert_ids)
        tables_b = slot_tables(ids[:, :, 2 * k : 3 * k], meta[:, :, 3 * k :], expert_ids)
        qkv_b = jnp.dot(h_b, w_qkv, preferred_element_type=jnp.float32).astype(jnp.bfloat16)
        early = (rows_a, mid_b, tables_a, tables_b, qkv_b)
        rows_a, sent_b, tables_a, tables_b, qkv_b = lax.optimization_barrier(early)
        rows_b = gather(sent_b)
        part_a = expert_sums(rows_a, tables_a, own, peer)
        sum_a = lax.psum_scatter(part_a, 'ep', axis_index_groups=groups)
        part_b = expert_sums(rows_b, tables_b, own, peer)
        out_b = ring_sum(part_b, mid_b, n_devs)
        out_a = (x_a.astype(jnp.float32) + sum_a).astype(jnp.bfloat16)
        return out_a, out_b, qkv_b

    row_spec = P(('dp', 'ep'), None)
    full_spec = P(None, None)
    expert_spec = P('ep', None, None)
    return jax.shard_map(
        local_step,
        mesh=mesh,
        in_specs=(row_spec, row_spec, row_spec, row_spec, row_spec, row_spec, row_spec, full_spec, full_spec, expert_spec, expert_spec, expert_spec),
        out_specs=(row_spec, row_spec, row_spec),
        check_vma=False,
    )
```

```python
import functools

import jax
import jax.numpy as jnp
from jax import lax
from jax.experimental import pallas as pl
from jax.experimental.pallas import tpu as pltpu
from jax.sharding import PartitionSpec as P

CORES = 2


def slot_tables(route_t, gate_t, expert_ids):
    n_src, top_k, tok_n = route_t.shape
    hit = route_t[:, :, None, :] == expert_ids[None, None, :, None]
    chosen = jnp.any(hit, axis=1)
    gate = jnp.sum(jnp.where(hit, gate_t[:, :, None, :], 0.0), axis=1)
    before = (jnp.arange(tok_n)[:, None] < jnp.arange(tok_n)[None, :]).astype(jnp.bfloat16)
    rank = jnp.einsum('set,tu->seu', chosen.astype(jnp.bfloat16), before, preferred_element_type=jnp.float32)
    rank = jnp.where(chosen, rank.astype(jnp.int32), -1)
    return rank, jnp.swapaxes(rank, 1, 2), jnp.swapaxes(gate, 1, 2)


def moe_kernel(n_src, local_n, capacity, n_x, rank_ref, rank_t_ref, gate_ref, *refs):
    x_refs, refs = refs[:n_x], refs[n_x:]
    own, peer = refs[0:3], refs[3:6]
    out_ref, rows_ref = refs[6], refs[7]
    bufs, sems = refs[8:11], refs[11]
    n_exp = CORES * local_n
    step = pl.program_id(0)
    tok_n, model_dim = rank_ref.shape[2], x_refs[0].shape[2]

    def load(side, idx, slot):
        for k in range(3):
            pltpu.make_async_copy(side[k].at[idx], bufs[k].at[slot], sems.at[slot, k]).start()

    @pl.when(step == 0)
    def _():
        load(own, 0, 0)
        load(own, 1, 1)

    @pl.when(step < n_src)
    def _():
        slot_no = lax.broadcasted_iota(jnp.int32, (capacity, tok_n), 0)
        picks = [jnp.where(slot_no == rank_ref[0, e : e + 1, :], 1.0, 0.0) for e in range(n_exp)]
        place = jnp.concatenate(picks, axis=0).astype(jnp.bfloat16)
        x = x_refs[0][0] if n_x == 1 else jnp.concatenate([x_ref[0] for x_ref in x_refs], axis=0)
        rows_ref[step] = jnp.dot(place, x, preferred_element_type=jnp.float32).astype(jnp.bfloat16)

    @pl.when(jnp.logical_and(step >= n_src, step < n_src + n_exp))
    def _():
        e = step - n_src
        slot = lax.rem(e, 2)
        for k in range(3):
            pltpu.make_async_copy(own[k].at[0], bufs[k].at[slot], sems.at[slot, k]).wait()
        at = pl.ds(pl.multiple_of(e * capacity, capacity), capacity)
        rows = rows_ref[:, at, :].reshape(n_src * capacity, model_dim)
        gate_act = jnp.dot(rows, bufs[0][slot], preferred_element_type=jnp.float32)
        up_act = jnp.dot(rows, bufs[1][slot], preferred_element_type=jnp.float32)
        hidden = (gate_act * jax.nn.sigmoid(gate_act) * up_act).astype(jnp.bfloat16)
        y = jnp.dot(hidden, bufs[2][slot], preferred_element_type=jnp.float32).astype(jnp.bfloat16)
        rows_ref[:, at, :] = y.reshape(n_src, capacity, model_dim)

        @pl.when(e + 2 < local_n)
        def _():
            load(own, e + 2, slot)

        @pl.when(jnp.logical_and(e + 2 >= local_n, e + 2 < n_exp))
        def _():
            load(peer, e + 2 - local_n, slot)

    @pl.when(step >= n_src + n_exp)
    def _():
        src = step - n_src - n_exp
        col = lax.broadcasted_iota(jnp.int32, (tok_n, capacity), 1)
        parts = []
        for e in range(n_exp):
            parts.append(jnp.where(col == rank_t_ref[0, :, e : e + 1], gate_ref[0, :, e : e + 1], 0.0))
        weight = jnp.concatenate(parts, axis=1)
        hi = weight.astype(jnp.bfloat16)
        rest = weight - hi.astype(jnp.float32)
        mid = rest.astype(jnp.bfloat16)
        lo = (rest - mid.astype(jnp.float32)).astype(jnp.bfloat16)
        y = rows_ref[src]
        total = jnp.dot(hi, y, preferred_element_type=jnp.float32)
        total += jnp.dot(mid, y, preferred_element_type=jnp.float32)
        total += jnp.dot(lo, y, preferred_element_type=jnp.float32)
        out_ref[0] = total


def expert_sums(rows, tables, own, peer):
    n_src, _, model_dim = rows[0].shape
    tok_n = sum(part.shape[1] for part in rows)
    local_n, _, ff_dim = own[0].shape
    n_exp = CORES * local_n
    rank, rank_t, gate = tables
    n_devs = n_src * CORES
    capacity = min(tok_n, 2 * ((tok_n * 8 + n_devs * local_n - 1) // (n_devs * local_n)))
    first = lambda i: (jnp.minimum(i, n_src - 1), 0, 0)
    last = lambda i: (jnp.clip(i - n_src - n_exp, 0, n_src - 1), 0, 0)
    any_spec = pl.BlockSpec(memory_space=pl.ANY)
    slots = n_exp * capacity
    flops = n_src * slots * model_dim * (6 * ff_dim + 2 * tok_n * 4)
    return pl.pallas_call(
        functools.partial(moe_kernel, n_src, local_n, capacity, len(rows)),
        grid=(n_src + n_exp + n_src,),
        out_shape=jax.ShapeDtypeStruct((n_src, tok_n, model_dim), jnp.float32),
        in_specs=[
            pl.BlockSpec((1, n_exp, tok_n), first),
            pl.BlockSpec((1, tok_n, n_exp), last),
            pl.BlockSpec((1, tok_n, n_exp), last),
        ]
        + [pl.BlockSpec((1, part.shape[1], model_dim), first) for part in rows]
        + [any_spec] * 6,
        out_specs=pl.BlockSpec((1, tok_n, model_dim), last),
        scratch_shapes=[
            pltpu.VMEM((n_src, slots, model_dim), jnp.bfloat16),
            pltpu.VMEM((2, model_dim, ff_dim), jnp.bfloat16),
            pltpu.VMEM((2, model_dim, ff_dim), jnp.bfloat16),
            pltpu.VMEM((2, ff_dim, model_dim), jnp.bfloat16),
            pltpu.SemaphoreType.DMA((2, 3)),
        ],
        compiler_params=pltpu.CompilerParams(
            dimension_semantics=('arbitrary',), vmem_limit_bytes=62 * 1024 * 1024
        ),
        cost_estimate=pl.CostEstimate(flops=flops, bytes_accessed=160 * 2**20, transcendentals=0),
    )(rank, rank_t, gate, *rows, *own, *peer)


def ring_kernel(n_src, n_devs, part_ref, mid_ref, out_ref, local, slots, load_sems, send_sems, recv_sems):
    tok_n, model_dim = mid_ref.shape
    rows_n, cols_n = tok_n // 2, model_dim // 2
    me = lax.axis_index('ep')
    pos = lax.div(me, CORES)
    to = {1: lax.rem(me + CORES, n_devs), -1: lax.rem(me + n_devs - CORES, n_devs)}

    barrier = pltpu.get_barrier_semaphore()
    for way in (1, -1):
        pl.semaphore_signal(barrier, inc=1, device_id={'ep': to[way]}, device_id_type=pl.DeviceIdType.MESH)
    pl.semaphore_wait(barrier, 2)

    far = n_src // 2
    near = n_src - 1 - far
    chains = []
    for dist, pairs in ((far, ((1, 0), (-1, 1))), (near, ((1, 1), (-1, 0)))):
        for r in range(2):
            for way, h in pairs:
                chains.append((way, r, h, dist))
    base, count = [], 0
    for chain in chains:
        base.append(count)
        count += chain[3]

    loads = {}
    order = sorted(range(n_src), key=lambda j: -min(j, n_src - j))
    for j in order:
        loads[j] = pltpu.make_async_copy(part_ref.at[lax.rem(pos + j, n_src)], local.at[j], load_sems.at[j])
        loads[j].start()
    ready = set()

    def mine(way, dist, r, h):
        j = (way * dist) % n_src
        if j not in ready:
            loads[j].wait()
            ready.add(j)
        return local.at[j, pl.ds(r * rows_n, rows_n), pl.ds(h * cols_n, cols_n)]

    copies = {}

    def send(c, hop, src):
        at = base[c] + hop - 1
        copies[c, hop] = pltpu.make_async_remote_copy(
            src_ref=src,
            dst_ref=slots.at[at],
            send_sem=send_sems.at[at],
            recv_sem=recv_sems.at[at],
            device_id={'ep': to[chains[c][0]]},
            device_id_type=pl.DeviceIdType.MESH,
        )
        copies[c, hop].start()

    for c, (way, r, h, dist) in enumerate(chains):
        send(c, 1, mine(way, dist, r, h))
    landed = {}
    for hop in range(1, far + 1):
        for c, (way, r, h, dist) in enumerate(chains):
            if hop > dist:
                continue
            copies[c, hop].wait_recv()
            here = slots.at[base[c] + hop - 1]
            if hop < dist:
                here[...] += mine(way, dist - hop, r, h)[...]
                send(c, hop + 1, here)
                continue
            if (r, h) not in landed:
                landed[r, h] = here
                continue
            total = mine(1, 0, r, h)[...] + (landed[r, h][...] + here[...])
            spot = (pl.ds(r * rows_n, rows_n), pl.ds(h * cols_n, cols_n))
            out_ref[spot] = (mid_ref[spot].astype(jnp.float32) + total).astype(jnp.bfloat16)
    for copy in copies.values():
        copy.wait_send()


def ring_sum(part, mid, n_devs):
    n_src, tok_n, model_dim = part.shape
    n_slots = 2 * 2 * (n_src - 1)
    vmem = pl.BlockSpec(memory_space=pltpu.VMEM)
    return pl.pallas_call(
        functools.partial(ring_kernel, n_src, n_devs),
        out_shape=jax.ShapeDtypeStruct((tok_n, model_dim), jnp.bfloat16),
        in_specs=[pl.BlockSpec(memory_space=pl.ANY), vmem],
        out_specs=vmem,
        scratch_shapes=[
            pltpu.VMEM((n_src, tok_n, model_dim), jnp.float32),
            pltpu.VMEM((n_slots, tok_n // 2, model_dim // 2), jnp.float32),
            pltpu.SemaphoreType.DMA((n_src,)),
            pltpu.SemaphoreType.DMA((n_slots,)),
            pltpu.SemaphoreType.DMA((n_slots,)),
        ],
        compiler_params=pltpu.CompilerParams(
            collective_id=0, has_side_effects=True, vmem_limit_bytes=56 * 1024 * 1024
        ),
        cost_estimate=pl.CostEstimate(flops=80 * 10**9, bytes_accessed=20 * 2**20, transcendentals=0),
    )(part, mid)


def spread_kernel(n_src, n_devs, x_ref, meta_ref, rows_ref, info_ref, send_sems, recv_sems):
    half = x_ref.shape[0] // 2
    me = lax.axis_index('ep')
    pos = lax.div(me, CORES)
    to = {1: lax.rem(me + CORES, n_devs), -1: lax.rem(me + n_devs - CORES, n_devs)}

    barrier = pltpu.get_barrier_semaphore()
    for way in (1, -1):
        pl.semaphore_signal(barrier, inc=1, device_id={'ep': to[way]}, device_id_type=pl.DeviceIdType.MESH)
    pl.semaphore_wait(barrier, 2)

    far = n_src // 2
    near = n_src - 1 - far
    cuts = [None, pl.ds(0, half), pl.ds(half, half)]
    chains = []
    for kind, longer in ((0, 1), (1, 1), (2, -1)):
        for way in (1, -1):
            chains.append((kind, way, far if way == longer else near))

    def place(kind, chip):
        return info_ref.at[chip] if kind == 0 else rows_ref.at[chip, cuts[kind]]

    copies = {}

    def send(c, hop, src):
        kind, way, _ = chains[c]
        chip = lax.rem(pos + n_src - way * (hop - 1), n_src)
        at = c * far + hop - 1
        copies[c, hop] = pltpu.make_async_remote_copy(
            src_ref=place(kind, chip) if src is None else src,
            dst_ref=place(kind, chip),
            send_sem=send_sems.at[at],
            recv_sem=recv_sems.at[at],
            device_id={'ep': to[way]},
            device_id_type=pl.DeviceIdType.MESH,
        )
        copies[c, hop].start()

    for c, (kind, way, dist) in enumerate(chains):
        send(c, 1, meta_ref if kind == 0 else x_ref.at[cuts[kind]])
    rows_ref[pos] = x_ref[...]
    info_ref[pos] = meta_ref[...]
    for hop in range(1, far + 1):
        for c, (kind, way, dist) in enumerate(chains):
            if hop > dist:
                continue
            copies[c, hop].wait_recv()
            if hop < dist:
                send(c, hop + 1, None)
    for copy in copies.values():
        copy.wait_send()


def spread(x, first_row, meta, n_devs):
    n_src = n_devs // CORES
    count, model_dim = x.shape[0] - first_row, x.shape[1]
    n_sems = 6 * (n_src // 2)
    vmem = pl.BlockSpec(memory_space=pltpu.VMEM)
    return pl.pallas_call(
        functools.partial(spread_kernel, n_src, n_devs),
        out_shape=(
            jax.ShapeDtypeStruct((n_src, count, model_dim), x.dtype),
            jax.ShapeDtypeStruct((n_src, *meta.shape), meta.dtype),
        ),
        in_specs=[vmem, vmem],
        out_specs=(vmem, vmem),
        scratch_shapes=[pltpu.SemaphoreType.DMA((n_sems,)), pltpu.SemaphoreType.DMA((n_sems,))],
        compiler_params=pltpu.CompilerParams(
            collective_id=1, has_side_effects=True, vmem_limit_bytes=16 * 1024 * 1024
        ),
        cost_estimate=pl.CostEstimate(flops=30 * 10**9, bytes_accessed=4 * 2**20, transcendentals=0),
    )(x[first_row:], meta)


def solution(mesh):
    n_devs = mesh.shape['ep']
    groups = [list(range(c, n_devs, CORES)) for c in range(CORES)]
    swap = [(d, d ^ 1) for d in range(n_devs)]

    def gather(vals):
        return lax.all_gather(vals, 'ep', axis_index_groups=groups)

    def local_step(x_a, route_a, gate_a, h_b, attn_b, route_b, gate_b, w_qkv, w_o, w_gate, w_up, w_down):
        k = route_a.shape[1]
        local_n = w_gate.shape[0]
        me = lax.axis_index('ep')
        own = (w_gate, w_up, w_down)
        split = x_a.shape[0] * 3 // 4
        rows_a = gather(x_a[:split])
        peer = tuple(lax.ppermute(w, 'ep', swap) for w in own)
        meta = [route_a.astype(jnp.float32), gate_a, route_b.astype(jnp.float32), gate_b]
        meta = jnp.concatenate([part.T for part in meta], axis=0)
        rest_a, meta = spread(x_a, split, meta, n_devs)
        proj_b = jnp.dot(attn_b, w_o, preferred_element_type=jnp.float32).astype(jnp.bfloat16)
        mid_b = (h_b.astype(jnp.float32) + proj_b.astype(jnp.float32)).astype(jnp.bfloat16)
        ids = meta.astype(jnp.int32)
        local = jnp.arange(local_n)
        expert_ids = jnp.concatenate([me * local_n + local, (me ^ 1) * local_n + local])
        tables_a = slot_tables(ids[:, :k], meta[:, k : 2 * k], expert_ids)
        tables_b = slot_tables(ids[:, 2 * k : 3 * k], meta[:, 3 * k :], expert_ids)
        early = (rows_a, mid_b, tables_a, tables_b)
        rows_a, sent_b, tables_a, tables_b = lax.optimization_barrier(early)
        rows_b = gather(sent_b)
        part_a = expert_sums((rows_a, rest_a), tables_a, own, peer)
        sum_a = lax.psum_scatter(part_a, 'ep', axis_index_groups=groups)
        part_b = expert_sums((rows_b,), tables_b, own, peer)
        part_b, after_b = lax.optimization_barrier((part_b, h_b))
        qkv_b = jnp.dot(after_b, w_qkv, preferred_element_type=jnp.float32).astype(jnp.bfloat16)
        part_b, qkv_b = lax.optimization_barrier((part_b, qkv_b))
        out_b = ring_sum(part_b, mid_b, n_devs)
        out_a = (x_a.astype(jnp.float32) + sum_a).astype(jnp.bfloat16)
        return out_a, out_b, qkv_b

    row_spec = P(('dp', 'ep'), None)
    full_spec = P(None, None)
    expert_spec = P('ep', None, None)
    return jax.shard_map(
        local_step,
        mesh=mesh,
        in_specs=(row_spec, row_spec, row_spec, row_spec, row_spec, row_spec, row_spec, full_spec, full_spec, expert_spec, expert_spec, expert_spec),
        out_specs=(row_spec, row_spec, row_spec),
        check_vma=False,
    )
```

```python
import functools

import jax
import jax.numpy as jnp
from jax import lax
from jax.experimental import pallas as pl
from jax.experimental.pallas import tpu as pltpu
from jax.sharding import PartitionSpec as P

CORES = 2


def slot_tables(route_t, gate_t, expert_ids):
    n_src, top_k, tok_n = route_t.shape
    hit = route_t[:, :, None, :] == expert_ids[None, None, :, None]
    chosen = jnp.any(hit, axis=1)
    gate = jnp.sum(jnp.where(hit, gate_t[:, :, None, :], 0.0), axis=1)
    before = (jnp.arange(tok_n)[:, None] < jnp.arange(tok_n)[None, :]).astype(jnp.bfloat16)
    rank = jnp.einsum('set,tu->seu', chosen.astype(jnp.bfloat16), before, preferred_element_type=jnp.float32)
    rank = jnp.where(chosen, rank.astype(jnp.int32), -1)
    return rank, jnp.swapaxes(rank, 1, 2), jnp.swapaxes(gate, 1, 2)


def moe_kernel(n_src, local_n, capacity, n_x, rank_ref, rank_t_ref, gate_ref, *refs):
    x_refs, refs = refs[:n_x], refs[n_x:]
    own, peer = refs[0:3], refs[3:6]
    out_ref, rows_ref = refs[6], refs[7]
    bufs, sems = refs[8:11], refs[11]
    n_exp = CORES * local_n
    step = pl.program_id(0)
    tok_n, model_dim = rank_ref.shape[2], x_refs[0].shape[2]

    def load(side, idx, slot):
        for k in range(3):
            pltpu.make_async_copy(side[k].at[idx], bufs[k].at[slot], sems.at[slot, k]).start()

    @pl.when(step == 0)
    def _():
        load(own, 0, 0)
        load(own, 1, 1)

    @pl.when(step < n_src)
    def _():
        slot_no = lax.broadcasted_iota(jnp.int32, (capacity, tok_n), 0)
        picks = [jnp.where(slot_no == rank_ref[0, e : e + 1, :], 1.0, 0.0) for e in range(n_exp)]
        place = jnp.concatenate(picks, axis=0).astype(jnp.bfloat16)
        x = x_refs[0][0] if n_x == 1 else jnp.concatenate([x_ref[0] for x_ref in x_refs], axis=0)
        rows_ref[step] = jnp.dot(place, x, preferred_element_type=jnp.float32).astype(jnp.bfloat16)

    @pl.when(jnp.logical_and(step >= n_src, step < n_src + n_exp))
    def _():
        e = step - n_src
        slot = lax.rem(e, 2)
        for k in range(3):
            pltpu.make_async_copy(own[k].at[0], bufs[k].at[slot], sems.at[slot, k]).wait()
        at = pl.ds(pl.multiple_of(e * capacity, capacity), capacity)
        rows = rows_ref[:, at, :].reshape(n_src * capacity, model_dim)
        gate_act = jnp.dot(rows, bufs[0][slot], preferred_element_type=jnp.float32)
        up_act = jnp.dot(rows, bufs[1][slot], preferred_element_type=jnp.float32)
        hidden = (gate_act * jax.nn.sigmoid(gate_act) * up_act).astype(jnp.bfloat16)
        y = jnp.dot(hidden, bufs[2][slot], preferred_element_type=jnp.float32).astype(jnp.bfloat16)
        rows_ref[:, at, :] = y.reshape(n_src, capacity, model_dim)

        @pl.when(e + 2 < local_n)
        def _():
            load(own, e + 2, slot)

        @pl.when(jnp.logical_and(e + 2 >= local_n, e + 2 < n_exp))
        def _():
            load(peer, e + 2 - local_n, slot)

    @pl.when(step >= n_src + n_exp)
    def _():
        src = step - n_src - n_exp
        col = lax.broadcasted_iota(jnp.int32, (tok_n, capacity), 1)
        parts = []
        for e in range(n_exp):
            parts.append(jnp.where(col == rank_t_ref[0, :, e : e + 1], gate_ref[0, :, e : e + 1], 0.0))
        weight = jnp.concatenate(parts, axis=1)
        hi = weight.astype(jnp.bfloat16)
        rest = weight - hi.astype(jnp.float32)
        mid = rest.astype(jnp.bfloat16)
        lo = (rest - mid.astype(jnp.float32)).astype(jnp.bfloat16)
        y = rows_ref[src]
        total = jnp.dot(hi, y, preferred_element_type=jnp.float32)
        total += jnp.dot(mid, y, preferred_element_type=jnp.float32)
        total += jnp.dot(lo, y, preferred_element_type=jnp.float32)
        out_ref[0] = total


def expert_sums(rows, tables, own, peer):
    n_src, _, model_dim = rows[0].shape
    tok_n = sum(part.shape[1] for part in rows)
    local_n, _, ff_dim = own[0].shape
    n_exp = CORES * local_n
    rank, rank_t, gate = tables
    n_devs = n_src * CORES
    capacity = min(tok_n, 2 * ((tok_n * 8 + n_devs * local_n - 1) // (n_devs * local_n)))
    first = lambda i: (jnp.minimum(i, n_src - 1), 0, 0)
    last = lambda i: (jnp.clip(i - n_src - n_exp, 0, n_src - 1), 0, 0)
    any_spec = pl.BlockSpec(memory_space=pl.ANY)
    slots = n_exp * capacity
    flops = n_src * slots * model_dim * (6 * ff_dim + 2 * tok_n * 4)
    return pl.pallas_call(
        functools.partial(moe_kernel, n_src, local_n, capacity, len(rows)),
        grid=(n_src + n_exp + n_src,),
        out_shape=jax.ShapeDtypeStruct((n_src, tok_n, model_dim), jnp.float32),
        in_specs=[
            pl.BlockSpec((1, n_exp, tok_n), first),
            pl.BlockSpec((1, tok_n, n_exp), last),
            pl.BlockSpec((1, tok_n, n_exp), last),
        ]
        + [pl.BlockSpec((1, part.shape[1], model_dim), first) for part in rows]
        + [any_spec] * 6,
        out_specs=pl.BlockSpec((1, tok_n, model_dim), last),
        scratch_shapes=[
            pltpu.VMEM((n_src, slots, model_dim), jnp.bfloat16),
            pltpu.VMEM((2, model_dim, ff_dim), jnp.bfloat16),
            pltpu.VMEM((2, model_dim, ff_dim), jnp.bfloat16),
            pltpu.VMEM((2, ff_dim, model_dim), jnp.bfloat16),
            pltpu.SemaphoreType.DMA((2, 3)),
        ],
        compiler_params=pltpu.CompilerParams(
            dimension_semantics=('arbitrary',), vmem_limit_bytes=62 * 1024 * 1024
        ),
        cost_estimate=pl.CostEstimate(flops=flops, bytes_accessed=160 * 2**20, transcendentals=0),
    )(rank, rank_t, gate, *rows, *own, *peer)


def ring_kernel(n_src, n_devs, part_ref, mid_ref, out_ref, local, slots, load_sems, send_sems, recv_sems):
    tok_n, model_dim = mid_ref.shape
    rows_n, cols_n = tok_n // 2, model_dim // 2
    me = lax.axis_index('ep')
    pos = lax.div(me, CORES)
    to = {1: lax.rem(me + CORES, n_devs), -1: lax.rem(me + n_devs - CORES, n_devs)}

    barrier = pltpu.get_barrier_semaphore()
    for way in (1, -1):
        pl.semaphore_signal(barrier, inc=1, device_id={'ep': to[way]}, device_id_type=pl.DeviceIdType.MESH)
    pl.semaphore_wait(barrier, 2)

    far = n_src // 2
    near = n_src - 1 - far
    chains = []
    for dist, pairs in ((far, ((1, 0), (-1, 1))), (near, ((1, 1), (-1, 0)))):
        for r in range(2):
            for way, h in pairs:
                chains.append((way, r, h, dist))
    base, count = [], 0
    for chain in chains:
        base.append(count)
        count += chain[3]

    loads = {}
    order = sorted(range(n_src), key=lambda j: -min(j, n_src - j))
    for j in order:
        loads[j] = pltpu.make_async_copy(part_ref.at[lax.rem(pos + j, n_src)], local.at[j], load_sems.at[j])
        loads[j].start()
    ready = set()

    def mine(way, dist, r, h):
        j = (way * dist) % n_src
        if j not in ready:
            loads[j].wait()
            ready.add(j)
        return local.at[j, pl.ds(r * rows_n, rows_n), pl.ds(h * cols_n, cols_n)]

    copies = {}

    def send(c, hop, src):
        at = base[c] + hop - 1
        copies[c, hop] = pltpu.make_async_remote_copy(
            src_ref=src,
            dst_ref=slots.at[at],
            send_sem=send_sems.at[at],
            recv_sem=recv_sems.at[at],
            device_id={'ep': to[chains[c][0]]},
            device_id_type=pl.DeviceIdType.MESH,
        )
        copies[c, hop].start()

    for c, (way, r, h, dist) in enumerate(chains):
        send(c, 1, mine(way, dist, r, h))
    landed = {}
    for hop in range(1, far + 1):
        for c, (way, r, h, dist) in enumerate(chains):
            if hop > dist:
                continue
            copies[c, hop].wait_recv()
            here = slots.at[base[c] + hop - 1]
            if hop < dist:
                here[...] += mine(way, dist - hop, r, h)[...]
                send(c, hop + 1, here)
                continue
            if (r, h) not in landed:
                landed[r, h] = here
                continue
            total = mine(1, 0, r, h)[...] + (landed[r, h][...] + here[...])
            spot = (pl.ds(r * rows_n, rows_n), pl.ds(h * cols_n, cols_n))
            out_ref[spot] = (mid_ref[spot].astype(jnp.float32) + total).astype(jnp.bfloat16)
    for copy in copies.values():
        copy.wait_send()


def ring_sum(part, mid, n_devs):
    n_src, tok_n, model_dim = part.shape
    n_slots = 2 * 2 * (n_src - 1)
    vmem = pl.BlockSpec(memory_space=pltpu.VMEM)
    return pl.pallas_call(
        functools.partial(ring_kernel, n_src, n_devs),
        out_shape=jax.ShapeDtypeStruct((tok_n, model_dim), jnp.bfloat16),
        in_specs=[pl.BlockSpec(memory_space=pl.ANY), vmem],
        out_specs=vmem,
        scratch_shapes=[
            pltpu.VMEM((n_src, tok_n, model_dim), jnp.float32),
            pltpu.VMEM((n_slots, tok_n // 2, model_dim // 2), jnp.float32),
            pltpu.SemaphoreType.DMA((n_src,)),
            pltpu.SemaphoreType.DMA((n_slots,)),
            pltpu.SemaphoreType.DMA((n_slots,)),
        ],
        compiler_params=pltpu.CompilerParams(
            collective_id=0, has_side_effects=True, vmem_limit_bytes=56 * 1024 * 1024
        ),
        cost_estimate=pl.CostEstimate(flops=80 * 10**9, bytes_accessed=20 * 2**20, transcendentals=0),
    )(part, mid)


def spread_kernel(n_src, n_devs, x_ref, meta_ref, rows_ref, info_ref, send_sems, recv_sems):
    half = x_ref.shape[0] // 2
    me = lax.axis_index('ep')
    pos = lax.div(me, CORES)
    to = {1: lax.rem(me + CORES, n_devs), -1: lax.rem(me + n_devs - CORES, n_devs)}

    barrier = pltpu.get_barrier_semaphore()
    for way in (1, -1):
        pl.semaphore_signal(barrier, inc=1, device_id={'ep': to[way]}, device_id_type=pl.DeviceIdType.MESH)
    pl.semaphore_wait(barrier, 2)

    far = n_src // 2
    near = n_src - 1 - far
    cuts = [None, pl.ds(0, half), pl.ds(half, half)]
    chains = []
    for kind, longer in ((0, 1), (1, 1), (2, -1)):
        for way in (1, -1):
            chains.append((kind, way, far if way == longer else near))

    def place(kind, chip):
        return info_ref.at[chip] if kind == 0 else rows_ref.at[chip, cuts[kind]]

    copies = {}

    def send(c, hop, src):
        kind, way, _ = chains[c]
        chip = lax.rem(pos + n_src - way * (hop - 1), n_src)
        at = c * far + hop - 1
        copies[c, hop] = pltpu.make_async_remote_copy(
            src_ref=place(kind, chip) if src is None else src,
            dst_ref=place(kind, chip),
            send_sem=send_sems.at[at],
            recv_sem=recv_sems.at[at],
            device_id={'ep': to[way]},
            device_id_type=pl.DeviceIdType.MESH,
        )
        copies[c, hop].start()

    for c, (kind, way, dist) in enumerate(chains):
        send(c, 1, meta_ref if kind == 0 else x_ref.at[cuts[kind]])
    rows_ref[pos] = x_ref[...]
    info_ref[pos] = meta_ref[...]
    for hop in range(1, far + 1):
        for c, (kind, way, dist) in enumerate(chains):
            if hop > dist:
                continue
            copies[c, hop].wait_recv()
            if hop < dist:
                send(c, hop + 1, None)
    for copy in copies.values():
        copy.wait_send()


def spread(x, first_row, meta, n_devs):
    n_src = n_devs // CORES
    count, model_dim = x.shape[0] - first_row, x.shape[1]
    n_sems = 6 * (n_src // 2)
    vmem = pl.BlockSpec(memory_space=pltpu.VMEM)
    return pl.pallas_call(
        functools.partial(spread_kernel, n_src, n_devs),
        out_shape=(
            jax.ShapeDtypeStruct((n_src, count, model_dim), x.dtype),
            jax.ShapeDtypeStruct((n_src, *meta.shape), meta.dtype),
        ),
        in_specs=[vmem, vmem],
        out_specs=(vmem, vmem),
        scratch_shapes=[pltpu.SemaphoreType.DMA((n_sems,)), pltpu.SemaphoreType.DMA((n_sems,))],
        compiler_params=pltpu.CompilerParams(
            collective_id=1, has_side_effects=True, vmem_limit_bytes=16 * 1024 * 1024
        ),
        cost_estimate=pl.CostEstimate(flops=30 * 10**9, bytes_accessed=4 * 2**20, transcendentals=0),
    )(x[first_row:], meta)


def solution(mesh):
    n_devs = mesh.shape['ep']
    groups = [list(range(c, n_devs, CORES)) for c in range(CORES)]
    swap = [(d, d ^ 1) for d in range(n_devs)]

    def gather(vals):
        return lax.all_gather(vals, 'ep', axis_index_groups=groups)

    def local_step(x_a, route_a, gate_a, h_b, attn_b, route_b, gate_b, w_qkv, w_o, w_gate, w_up, w_down):
        k = route_a.shape[1]
        local_n = w_gate.shape[0]
        me = lax.axis_index('ep')
        own = (w_gate, w_up, w_down)
        split = x_a.shape[0] * 3 // 4
        rows_a = gather(x_a[:split])
        peer = tuple(lax.ppermute(w, 'ep', swap) for w in own)
        meta = [route_a.astype(jnp.float32), gate_a, route_b.astype(jnp.float32), gate_b]
        meta = jnp.concatenate([part.T for part in meta], axis=0)
        rest_a, meta = spread(x_a, split, meta, n_devs)
        proj_b = jnp.dot(attn_b, w_o, preferred_element_type=jnp.float32).astype(jnp.bfloat16)
        mid_b = (h_b.astype(jnp.float32) + proj_b.astype(jnp.float32)).astype(jnp.bfloat16)
        ids = meta.astype(jnp.int32)
        local = jnp.arange(local_n)
        expert_ids = jnp.concatenate([me * local_n + local, (me ^ 1) * local_n + local])
        tables_a = slot_tables(ids[:, :k], meta[:, k : 2 * k], expert_ids)
        tables_b = slot_tables(ids[:, 2 * k : 3 * k], meta[:, 3 * k :], expert_ids)
        qkv_b = jnp.dot(h_b, w_qkv, preferred_element_type=jnp.float32).astype(jnp.bfloat16)
        early = (rows_a, mid_b, tables_a, tables_b, qkv_b)
        rows_a, sent_b, tables_a, tables_b, qkv_b = lax.optimization_barrier(early)
        rows_b = gather(sent_b)
        part_a = expert_sums((rows_a, rest_a), tables_a, own, peer)
        sum_a = lax.psum_scatter(part_a, 'ep', axis_index_groups=groups)
        part_b = expert_sums((rows_b,), tables_b, own, peer)
        out_b = ring_sum(part_b, mid_b, n_devs)
        out_a = (x_a.astype(jnp.float32) + sum_a).astype(jnp.bfloat16)
        return out_a, out_b, qkv_b

    row_spec = P(('dp', 'ep'), None)
    full_spec = P(None, None)
    expert_spec = P('ep', None, None)
    return jax.shard_map(
        local_step,
        mesh=mesh,
        in_specs=(row_spec, row_spec, row_spec, row_spec, row_spec, row_spec, row_spec, full_spec, full_spec, expert_spec, expert_spec, expert_spec),
        out_specs=(row_spec, row_spec, row_spec),
        check_vma=False,
    )
```
